512 devices in a mesh: gx: 8 (over z), gy: 4 (over x), gz: 16 (over y, core).
Axes of the slice: x: 4, y: 8, z: 8, core: 2. Of those that a mesh axis runs over, the one named last changes fastest.
Arguments:
- right_side: float32 [64, 64, 2048], P('gx', 'gy', 'gz'), may hold values from -40 to 40
- fiber_class: int32 [64, 64, 2048], P('gx', 'gy', 'gz'), may hold values from 0 to 15
- conductivity_scale: float32 [64, 64, 2048], P('gx', 'gy', 'gz'), may hold values from 0.8 to 1.25
- class_tensor: float32 [6, 16], replicated, may hold values from -0.15 to 1.8, as said below
- block_ids: int32 [8, 4, 32], replicated, may hold values from 0 to 63, as said below
Outputs:
- solution: float32 [64, 64, 2048], P('gx', 'gy', 'gz')
- residual: float32 [64, 64, 2048], P('gx', 'gy', 'gz')
The draws below stay inside these ranges and needn't reach their ends.
Inputs may be any that keep to these rules, and one draw needn't show every extreme that they name: `class_tensor`: column k is the tensor t I + (l - t) f f^T for a unit vector f, with 1 <= t <= 1.5 and 1.05 <= l / t <= 1.2. `block_ids`: each subdomain number names exactly 16 blocks.
All inputs are finite; a program needn't handle non-finite values.
Results may differ from the reference program's by a relative error of at most 0.0003.
Values sent between devices are 32-bit elements; how exact they have to be, the bound alone decides.
No kernel may reach another device: no remote copies, remote signals or barrier semaphores. Data moves between devices by JAX's collectives and lax.ppermute only.
A program may use at most 64 MiB of HBM per device.

```python
import math
import jax
import jax.numpy as jnp
from jax import lax

CX = 8
CY = 16
BZ = 64
COARSE = 64
NCLS = 16
ITERS = 2
NX = 64
NY = 64
NZ = 2048
NBX = 8
NBY = 4
NBZ = 32


def draw_right_side(key, part):
    noise_key, spread_key = jax.random.split(jax.random.fold_in(key, 11))
    shape = (NX, NY, NZ)
    depth = (jnp.arange(NZ, dtype=jnp.float32) + 0.5) / NZ
    ramp = (1.0 + 2.0 * depth)[None, None, :]
    noise = jax.random.truncated_normal(noise_key, -4.0, 4.0, shape, jnp.float32)
    spread = jnp.exp(jax.random.uniform(spread_key, shape, jnp.float32, 0.0, math.log(10.0)))
    return (0.3 * noise * spread * ramp).astype(jnp.float32)


def draw_class_tensor(key, part):
    keys = jax.random.split(jax.random.fold_in(key, 23), 4)
    azimuth = jax.random.uniform(keys[0], (NCLS,), jnp.float32, -math.pi, math.pi)
    elevation = jax.random.uniform(keys[1], (NCLS,), jnp.float32, -0.5 * math.pi, 0.5 * math.pi)
    transverse = jnp.exp(jax.random.uniform(keys[2], (NCLS,), jnp.float32, 0.0, math.log(1.5)))
    anisotropy = jnp.exp(jax.random.uniform(keys[3], (NCLS,), jnp.float32, math.log(1.05), math.log(1.2)))
    excess = transverse * (anisotropy - 1.0)
    fiber_x = jnp.cos(elevation) * jnp.cos(azimuth)
    fiber_y = jnp.cos(elevation) * jnp.sin(azimuth)
    fiber_z = jnp.sin(elevation)
    rows = [transverse + excess * fiber_x * fiber_x, transverse + excess * fiber_y * fiber_y, transverse + excess * fiber_z * fiber_z, excess * fiber_x * fiber_y, excess * fiber_x * fiber_z, excess * fiber_y * fiber_z]
    return jnp.stack(rows).astype(jnp.float32)


def draw_block_ids(key, part):
    order = jax.random.permutation(jax.random.fold_in(key, 37), NBX * NBY * NBZ)
    return (order % COARSE).astype(jnp.int32).reshape(NBX, NBY, NBZ)


def set_ends(array, stream_key, low, largest):
    spot = [jax.random.randint(jax.random.fold_in(stream_key, axis), (), 0, length) for axis, length in enumerate(array.shape)]
    longest = array.shape.index(max(array.shape))
    beside = spot[:longest] + [(spot[longest] + 1) % array.shape[longest]] + spot[longest + 1:]
    return array.at[tuple(spot)].set(low).at[tuple(beside)].set(largest)


def level_of(stream_key, shape, shards, low, top_value):
    def one(dim, shards_of):
        heights = jax.random.uniform(jax.random.fold_in(jax.random.fold_in(stream_key, 6), dim), (shards_of,), jnp.float32, low / len(shards), top_value / len(shards))
        return jnp.repeat(jnp.exp(heights), shape[dim] // shards_of).reshape((-1,) + (1,) * (len(shape) - dim - 1))

    gain = one(*shards[0])
    for cut in shards[1:]:
        gain = gain * one(*cut)
    return gain


def setup_inputs(seed: int = 0) -> dict:
    seeds = jax.random.split(jax.random.key(seed), 6)
    right_side = draw_right_side(jax.random.fold_in(seeds[5], 71), 0)
    fiber_class = set_ends(jax.random.randint(seeds[1], (NX, NY, NZ), 0, NCLS), jax.random.fold_in(seeds[1], 1), 0, NCLS - 1).astype(jnp.int32)
    conductivity_scale = jnp.clip(jnp.exp(math.log(1.25) - 0.4462871 * jax.random.uniform(seeds[2], (NX, NY, NZ), jnp.float32) ** level_of(seeds[2], (NX, NY, NZ), ((0, 8), (1, 4), (2, 16)), -0.2, 0.2)), 0.8, 1.25)
    class_tensor = draw_class_tensor(jax.random.fold_in(seeds[5], 71), 0)
    block_ids = draw_block_ids(jax.random.fold_in(seeds[5], 71), 0)
    return dict(right_side=right_side, fiber_class=fiber_class, conductivity_scale=conductivity_scale, class_tensor=class_tensor, block_ids=block_ids)


STENCIL_TAPS = ((1, 0, 0, 0, 1.0), (-1, 0, 0, 0, 1.0), (0, 1, 0, 1, 1.0), (0, -1, 0, 1, 1.0), (0, 0, 1, 2, 1.0), (0, 0, -1, 2, 1.0), (1, 1, 0, 3, 0.5), (-1, -1, 0, 3, 0.5), (1, -1, 0, 3, -0.5), (-1, 1, 0, 3, -0.5), (1, 0, 1, 4, 0.5), (-1, 0, -1, 4, 0.5), (1, 0, -1, 4, -0.5), (-1, 0, 1, 4, -0.5), (0, 1, 1, 5, 0.5), (0, -1, -1, 5, 0.5), (0, 1, -1, 5, -0.5), (0, -1, 1, 5, -0.5))

def shifted(padded, step_x, step_y, step_z):
    width_x = padded.shape[-3] - 2
    width_y = padded.shape[-2] - 2
    width_z = padded.shape[-1] - 2
    return padded[1 + step_x:1 + step_x + width_x, 1 + step_y:1 + step_y + width_y, 1 + step_z:1 + step_z + width_z]

def edge_weights(tensors, step_x, step_y, step_z, component, factor):
    layer = tensors[component]
    return 0.5 * factor * (shifted(layer, 0, 0, 0) + shifted(layer, step_x, step_y, step_z))

def operate(padded, tensors):
    centre = shifted(padded, 0, 0, 0)
    accumulated = jnp.zeros_like(centre)
    for step_x, step_y, step_z, component, factor in STENCIL_TAPS:
        weight = edge_weights(tensors, step_x, step_y, step_z, component, factor)
        accumulated = accumulated + weight * (centre - shifted(padded, step_x, step_y, step_z))
    return accumulated

def class_onehot(labels, count):
    return (labels[..., None] == jnp.arange(count, dtype=jnp.int32)).astype(jnp.float32)

def reach_onehot(length, offset):
    position = jnp.arange(length, dtype=jnp.int32)
    relative = (position + offset) // length + 1
    return (relative[:, None] == jnp.arange(3, dtype=jnp.int32)[None, :]).astype(jnp.float32)

def centre_mask():
    places = jnp.arange(3, dtype=jnp.int32)
    return (places[:, None, None] == 1) & (places[None, :, None] == 1) & (places[None, None, :] == 1)

def tensor_grid(fiber_class, conductivity_scale, class_tensor):
    return tuple((jnp.pad(class_tensor[component][fiber_class] * conductivity_scale, 1) for component in range(6)))

def coarse_matrix(tensors, block_ids):
    highest = lax.Precision.HIGHEST
    rim_weight = jnp.zeros((NBX, NBY, NBZ, 3, 3, 3), jnp.float32)
    for step_x, step_y, step_z, component, factor in STENCIL_TAPS:
        weight = edge_weights(tensors, step_x, step_y, step_z, component, factor)
        weight = weight.reshape(NBX, CX, NBY, CY, NBZ, BZ)
        rim_weight = rim_weight + jnp.einsum('axbycz,xd,ye,zf->abcdef', weight, reach_onehot(CX, step_x), reach_onehot(CY, step_y), reach_onehot(BZ, step_z), precision=highest)
    rim_weight = jnp.where(centre_mask()[None, None, None], 0.0, rim_weight)
    own_hot = class_onehot(block_ids, COARSE)
    padded_ids = jnp.pad(block_ids, 1, constant_values=-1)
    diagonal_terms = jnp.einsum('abck,abc->k', own_hot, jnp.sum(rim_weight, axis=(3, 4, 5)), precision=highest)
    coupling = jnp.zeros((COARSE, COARSE), jnp.float32)
    for off_x in range(3):
        for off_y in range(3):
            for off_z in range(3):
                if off_x == 1 and off_y == 1 and (off_z == 1):
                    continue
                neighbours = padded_ids[off_x:off_x + NBX, off_y:off_y + NBY, off_z:off_z + NBZ]
                coupling = coupling + jnp.einsum('abck,abc,abcl->kl', own_hot, rim_weight[:, :, :, off_x, off_y, off_z], class_onehot(neighbours, COARSE), precision=highest)
    matrix = jnp.diag(diagonal_terms) - coupling
    return 0.5 * (matrix + matrix.T)

def reference(right_side, fiber_class, conductivity_scale, class_tensor, block_ids):
    highest = lax.Precision.HIGHEST
    tensors = tensor_grid(fiber_class, conductivity_scale, class_tensor)
    coarse = coarse_matrix(tensors, block_ids)
    own_hot = class_onehot(block_ids, COARSE)

    def apply_field(field):
        return operate(jnp.pad(field, 1), tensors)

    def restrict(field):
        block_totals = jnp.sum(field.reshape(NBX, CX, NBY, CY, NBZ, BZ), axis=(1, 3, 5))
        return jnp.einsum('abck,abc->k', own_hot, block_totals, precision=highest)

    def prolong(coarse_values):
        per_block = jnp.einsum('abck,k->abc', own_hot, coarse_values, precision=highest)
        return jnp.broadcast_to(per_block[:, None, :, None, :, None], (NBX, CX, NBY, CY, NBZ, BZ)).reshape(NX, NY, NZ)

    def coarse_solve(field):
        return jnp.linalg.solve(coarse, restrict(field))
    coarse_part = prolong(coarse_solve(right_side))
    residual = right_side - apply_field(coarse_part)
    direction = residual
    norm_now = jnp.sum(residual * residual)
    estimate = jnp.zeros_like(right_side)
    for iteration in range(ITERS):
        product = apply_field(direction)
        image_field = product - apply_field(prolong(coarse_solve(product)))
        step_size = norm_now / jnp.sum(direction * image_field)
        estimate = estimate + step_size * direction
        residual = residual - step_size * image_field
        if iteration + 1 < ITERS:
            norm_next = jnp.sum(residual * residual)
            direction = residual + norm_next / norm_now * direction
            norm_now = norm_next
    solution = coarse_part + estimate - prolong(coarse_solve(apply_field(estimate)))
    return (solution, residual)
```

```python
import functools

import jax
import jax.numpy as jnp
import numpy as np
from jax import lax
from jax.experimental import pallas as pl
from jax.experimental.pallas import tpu as pltpu
from jax.sharding import PartitionSpec as P

COARSE = 64
NCLS = 16
ZBLK = 2
HALO = 3
LANES = 128
EY = 24
EZ = 256
SLOTS = 32
HIGHEST = lax.Precision.HIGHEST

STENCIL_TAPS = (
    (1, 0, 0, 0, 1.0),
    (-1, 0, 0, 0, 1.0),
    (0, 1, 0, 1, 1.0),
    (0, -1, 0, 1, 1.0),
    (0, 0, 1, 2, 1.0),
    (0, 0, -1, 2, 1.0),
    (1, 1, 0, 3, 0.5),
    (-1, -1, 0, 3, 0.5),
    (1, -1, 0, 3, -0.5),
    (-1, 1, 0, 3, -0.5),
    (1, 0, 1, 4, 0.5),
    (-1, 0, -1, 4, 0.5),
    (1, 0, -1, 4, -0.5),
    (-1, 0, 1, 4, -0.5),
    (0, 1, 1, 5, 0.5),
    (0, -1, -1, 5, 0.5),
    (0, 1, -1, 5, -0.5),
    (0, -1, 1, 5, -0.5),
)
EDGES = (
    (1, 0, 0, 0, 1.0),
    (0, 1, 0, 1, 1.0),
    (0, 0, 1, 2, 1.0),
    (1, 1, 0, 3, 0.5),
    (1, -1, 0, 3, -0.5),
    (1, 0, 1, 4, 0.5),
    (1, 0, -1, 4, -0.5),
    (0, 1, 1, 5, 0.5),
    (0, 1, -1, 5, -0.5),
)
NEIGHBOURS = tuple(
    (a, b, c)
    for a in (-1, 0, 1)
    for b in (-1, 0, 1)
    for c in (-1, 0, 1)
    if 1 <= abs(a) + abs(b) + abs(c) <= 2
)
NNB = len(NEIGHBOURS)
RHS_SLOT = NNB
ROWS = 56
VMEM = pl.BlockSpec(memory_space=pltpu.VMEM)
SMEM = pl.BlockSpec(memory_space=pltpu.SMEM)


def crossing_table():
    table = np.zeros((3, SLOTS, ROWS), np.float32)

    def cells(step, reach):
        if step == 0:
            return ((2, 1.0),) if reach == 0 else ()
        edge = 1 if step > 0 else 0
        if reach == step:
            return ((edge, 1.0),)
        return ((2, 1.0), (edge, -1.0)) if reach == 0 else ()

    for sx, sy, sz, component, factor in STENCIL_TAPS:
        for slot, (a, b, c) in enumerate(NEIGHBOURS):
            for px, fx in cells(sx, a):
                for py, fy in cells(sy, b):
                    for pz, fz in cells(sz, c):
                        table[pz, slot, component * 9 + px * 3 + py] += 0.5 * factor * fx * fy * fz
    table[2, RHS_SLOT, 54] = 1.0
    return table.reshape(3 * SLOTS, ROWS)


def lookup(kinds, scale, table):
    values = [jnp.full(scale.shape, table[c, 0], jnp.float32) for c in range(6)]
    for kind in range(1, NCLS):
        hit = kinds == kind
        values = [jnp.where(hit, table[c, kind], values[c]) for c in range(6)]
    return [value * scale for value in values]


def lane_ids(shape):
    return lax.broadcasted_iota(jnp.int32, shape, len(shape) - 1)


def row_ids(shape):
    return lax.broadcasted_iota(jnp.int32, shape, len(shape) - 2)


def own_sums_kernel(table_ref, source_ref, kinds_ref, scale_ref, crossing_ref, out_ref, rows_ref):
    cx, cy, cz = source_ref.shape
    rows_ref[...] = jnp.zeros_like(rows_ref)
    firsts, totals = None, None
    total_source = None
    for x in range(cx):
        layers = lookup(kinds_ref[x], scale_ref[x], table_ref)
        total_source = source_ref[x] if x == 0 else total_source + source_ref[x]
        if x == 0:
            firsts, totals = layers, layers
        else:
            totals = [t + v for t, v in zip(totals, layers)]
    for c in range(6):
        for px, field in enumerate((firsts[c], layers[c], totals[c])):
            at = c * 9 + px * 3
            rows_ref[at : at + 1, :] = field[0:1]
            rows_ref[at + 1 : at + 2, :] = field[cy - 1 : cy]
            rows_ref[at + 2 : at + 3, :] = jnp.sum(field, axis=0, keepdims=True)
    rows_ref[54:55, :] = jnp.sum(total_source, axis=0, keepdims=True)
    sums = jnp.dot(crossing_ref[...], rows_ref[...], precision=HIGHEST, preferred_element_type=jnp.float32)
    block = cz // ZBLK
    lane = lane_ids((SLOTS, cz))
    picked = (
        jnp.where(lane % block == 0, sums[:SLOTS], 0.0)
        + jnp.where(lane % block == block - 1, sums[SLOTS : 2 * SLOTS], 0.0)
        + sums[2 * SLOTS :]
    )
    spread = jnp.concatenate([picked] * ZBLK + [jnp.zeros((LANES - ZBLK * SLOTS, cz), jnp.float32)], axis=0)
    group = row_ids((LANES, cz)) // SLOTS
    spread = jnp.where(lane_ids((LANES, cz)) // block == group, spread, 0.0)
    row = lax.dot_general(
        jnp.ones((8, cz), jnp.float32), spread, (((1,), (1,)), ((), ())),
        precision=HIGHEST, preferred_element_type=jnp.float32,
    )
    out_ref[...] = jnp.broadcast_to(row[0:1].reshape(1, 1, LANES), out_ref.shape)


def shift_z(x, step):
    return pltpu.roll(x, (-step) % EZ, 1)


def shift_y(x, step):
    return pltpu.roll(x, (-step) % EY, 0)


def shift(x, step_y, step_z):
    if step_y:
        x = shift_y(x, step_y)
    if step_z:
        x = shift_z(x, step_z)
    return x


def weights_kernel(table_ref, kinds_ref, scale_ref, out_ref, layers_ref):
    planes = scale_ref.shape[0]

    def fill(p, carry):
        for c, layer in enumerate(lookup(kinds_ref[p], scale_ref[p], table_ref)):
            layers_ref[c, p] = layer
        return carry

    lax.fori_loop(0, planes, fill, 0)

    def edges(p, carry):
        after = jnp.minimum(p + 1, planes - 1)
        for e, (sx, sy, sz, c, factor) in enumerate(EDGES):
            beside = layers_ref[c, after] if sx else layers_ref[c, p]
            out_ref[e, p] = (0.5 * factor) * (layers_ref[c, p] + shift(beside, sy, sz))
        return carry

    lax.fori_loop(0, planes, edges, 0)


def across(here, after, weights, p):
    g1 = weights[0, p] * (here - after)
    g2 = weights[3, p] * (here - shift_y(after, 1))
    g3 = weights[4, p] * (here - shift_y(after, -1))
    g4 = weights[5, p] * (here - shift_z(after, 1))
    g5 = weights[6, p] * (here - shift_z(after, -1))
    leaving = (g1 + g2) + (g3 + g4) + g5
    arriving = (g1 + shift_y(g2, -1)) + (shift_y(g3, 1) + shift_z(g4, -1)) + shift_z(g5, 1)
    return leaving, arriving


def within(here, weights, p):
    up = shift_y(here, 1)
    h1 = weights[1, p] * (here - up)
    h2 = weights[2, p] * (here - shift_z(here, 1))
    h3 = weights[7, p] * (here - shift_z(up, 1))
    h4 = weights[8, p] * (here - shift_z(up, -1))
    back = shift_y(h1 + shift_z(h3, -1) + shift_z(h4, 1), -1) + shift_z(h2, -1)
    return (h1 + h2) + (h3 + h4) - back


def operate(plane, weights, low, high, emit):
    _, arriving = across(plane(low - 1), plane(low), weights, low - 1)
    for p in range(low, high):
        here = plane(p)
        leaving, coming = across(here, plane(p + 1), weights, p)
        emit(p, within(here, weights, p) + leaving - arriving)
        arriving = coming


def column_of(inverse, row):
    return jnp.sum(inverse * row, axis=1, keepdims=True)


def spread_planes(column, ids_ref):
    coarse = column.shape[0]
    wide = jnp.broadcast_to(column, (coarse, EZ))
    label = row_ids((coarse, EZ))
    row = row_ids((EY, EZ))
    cy = EY - 8
    planes = []
    for a in range(3):
        before, own, after = (
            jnp.sum(jnp.where(ids_ref[3 * a + b : 3 * a + b + 1, :] == label, wide, 0.0), axis=0, keepdims=True)
            for b in range(3)
        )
        planes.append(jnp.where(row < cy, own, jnp.where(row < cy + 4, after, before)))
    return planes


def by_plane(planes, cx):
    return lambda p: planes[0] if p < HALO else planes[1] if p < HALO + cx else planes[2]


def labelled_row(totals, norm, cross, ids_ref):
    lane = lane_ids((1, LANES))
    block = LANES // ZBLK
    row = jnp.where(lane == COARSE, jnp.sum(norm, keepdims=True).reshape(1, 1), 0.0)
    row = row + jnp.where(lane == COARSE + 1, jnp.sum(cross, keepdims=True).reshape(1, 1), 0.0)
    for j in range(ZBLK):
        total = jnp.sum(jnp.where(lane // block == j, totals, 0.0), axis=1, keepdims=True)
        label = ids_ref[4:5, j * block : j * block + 1]
        row = row + jnp.where(lane == label, total, 0.0)
    return row


def own_part(plane, cy, cz):
    return plane[:cy, :cz]


def coarse_kernel(rows_ref, ids_ref, near_ref, inverse_ref, rhs_ref):
    count = rows_ref.shape[0] * rows_ref.shape[1]
    flat = rows_ref[...].reshape(count, LANES)
    features = flat.T
    coarse = inverse_ref.shape[0]
    label = row_ids((coarse, count))
    slot_row = row_ids((SLOTS, count))
    packed = None
    for g in range(LANES // SLOTS):
        part = features[g * SLOTS : (g + 1) * SLOTS]
        reach = None
        for s in range(NNB):
            term = jnp.where(near_ref[g, s : s + 1, :] == label, part[s : s + 1], 0.0)
            reach = term if s == 0 else reach + term
        crossing = jnp.sum(jnp.where(slot_row < NNB, part, 0.0), axis=0, keepdims=True)
        sub = row_ids((8, count))
        extra = jnp.where(sub == 0, crossing, jnp.where(sub == 1, part[RHS_SLOT : RHS_SLOT + 1], 0.0))
        own = jnp.where(ids_ref[g : g + 1, :] == label, 1.0, 0.0)
        product = lax.dot_general(
            jnp.concatenate([reach, extra], axis=0), own, (((1,), (1,)), ((), ())),
            precision=HIGHEST, preferred_element_type=jnp.float32,
        )
        packed = product if g == 0 else packed + product
    coupling = packed[:coarse]
    mirrored = coupling.T
    row = row_ids((coarse, coarse))
    lane = lane_ids((coarse, coarse))
    diagonal = packed[coarse : coarse + 1] + jnp.sum(mirrored, axis=0, keepdims=True)
    matrix = jnp.where(row == lane, diagonal, 0.0) - (coupling + mirrored)
    for k in range(coarse):
        pivot_row = matrix[k : k + 1, :]
        column = matrix[:, k : k + 1]
        scaled = pivot_row / matrix[k : k + 1, k : k + 1]
        inverse_pivot = 1.0 / matrix[k : k + 1, k : k + 1]
        rest = matrix - column * scaled
        rest = jnp.where(lane == k, -column * inverse_pivot, rest)
        scaled = jnp.where(lane[k : k + 1] == k, inverse_pivot, scaled)
        matrix = jnp.where(row == k, scaled, rest)
    inverse_ref[...] = jnp.concatenate([matrix, jnp.zeros((coarse, LANES - coarse), jnp.float32)], axis=1)
    rhs_ref[...] = jnp.concatenate(
        [packed[coarse + 1 : coarse + 2], jnp.zeros((1, LANES - coarse), jnp.float32)], axis=1
    )


def first_kernel(weights_ref, source_ref, scale_ref, ids_ref, inverse_ref, rhs_ref,
                 residual_ref, image_ref, row_ref, column_ref):
    planes = source_ref.shape[0]
    cx, cy, cz = planes - 2 * HALO, EY - 8, LANES
    column = column_of(inverse_ref[...], rhs_ref[...])
    column_ref[...] = jnp.broadcast_to(column, column_ref.shape)
    residual_ref[0] = jnp.zeros((EY, EZ), jnp.float32)
    residual_ref[planes - 1] = jnp.zeros((EY, EZ), jnp.float32)

    def residual(p, image):
        residual_ref[p] = jnp.where(scale_ref[p] != 0.0, source_ref[p] - image, 0.0)

    operate(by_plane(spread_planes(column, ids_ref), cx), weights_ref, 1, planes - 1, residual)
    sums = [jnp.zeros((cy, cz), jnp.float32)] * 3

    def image(p, value):
        image_ref[p] = value
        if HALO <= p < HALO + cx:
            mine, field = own_part(value, cy, cz), own_part(residual_ref[p], cy, cz)
            sums[0] = sums[0] + mine
            sums[1] = sums[1] + field * field
            sums[2] = sums[2] + field * mine

    operate(lambda p: residual_ref[p], weights_ref, 2, planes - 2, image)
    row = labelled_row(jnp.sum(sums[0], axis=0, keepdims=True), sums[1], sums[2], ids_ref)
    row_ref[...] = jnp.broadcast_to(row.reshape(1, 1, LANES), row_ref.shape)


def second_kernel(weights_ref, scale_ref, residual_ref, image_ref, ids_ref, inverse_ref, sums_ref,
                  next_ref, product_ref, along_ref, row_ref, column_ref, scalars_ref, field_ref):
    planes = scale_ref.shape[0]
    cx, cy, cz = planes - 2 * HALO, EY - 8, LANES
    totals = jnp.sum(sums_ref[...], axis=0)
    column = column_of(inverse_ref[...], totals)
    column_ref[...] = jnp.broadcast_to(column, column_ref.shape)
    correction = jnp.sum(inverse_ref[...] * column, axis=0, keepdims=True)
    lane = lane_ids((1, LANES))
    inverse = inverse_ref[...]
    bent = jnp.sum(column * jnp.sum(jnp.where(lane_ids(inverse.shape) == row_ids(inverse.shape), totals, 0.0), axis=1, keepdims=True), axis=0, keepdims=True)
    norm = jnp.sum(jnp.where(lane == COARSE, totals, 0.0), axis=1, keepdims=True)
    cross = jnp.sum(jnp.where(lane == COARSE + 1, totals, 0.0), axis=1, keepdims=True)
    step = norm / (cross - bent)
    sub = row_ids((8, LANES))
    scalars_ref[...] = jnp.where(sub == 0, norm, jnp.where(sub == 1, step, 0.0))

    def follow(p, value):
        value = image_ref[p] - value
        if HALO <= p < HALO + cx:
            along_ref[p - HALO] = own_part(value, cy, cz)
        updated = jnp.where(scale_ref[p] != 0.0, residual_ref[p] - step * value, 0.0)
        field_ref[p] = updated
        if HALO <= p < HALO + cx:
            next_ref[p - HALO] = own_part(updated, cy, cz)

    operate(by_plane(spread_planes(column, ids_ref), cx), weights_ref, 2, planes - 2, follow)
    sums = [jnp.zeros((cy, cz), jnp.float32)] * 3

    def image(p, value):
        mine, field = own_part(value, cy, cz), own_part(field_ref[p], cy, cz)
        product_ref[p - HALO] = mine
        sums[0] = sums[0] + mine
        sums[1] = sums[1] + field * field
        sums[2] = sums[2] + field * mine

    operate(lambda p: field_ref[p], weights_ref, HALO, planes - HALO, image)
    row = labelled_row(jnp.sum(sums[0], axis=0, keepdims=True), sums[1], sums[2], ids_ref)
    row_ref[...] = jnp.broadcast_to(row.reshape(1, 1, LANES), row_ref.shape)


def last_kernel(weights_ref, residual_ref, next_ref, product_ref, along_ref, ids_ref, inverse_ref, sums_ref,
                scalars_ref, first_ref, second_ref, solution_ref, final_ref):
    cx, cy, cz = next_ref.shape
    planes = cx + 2 * HALO
    totals = jnp.sum(sums_ref[...], axis=0)
    inverse = inverse_ref[...]
    column = column_of(inverse, totals)
    lane = lane_ids((1, LANES))
    bent = jnp.sum(column * jnp.sum(jnp.where(lane_ids(inverse.shape) == row_ids(inverse.shape), totals, 0.0), axis=1, keepdims=True), axis=0, keepdims=True)
    norm = jnp.sum(jnp.where(lane == COARSE, totals, 0.0), axis=1, keepdims=True)
    cross = jnp.sum(jnp.where(lane == COARSE + 1, totals, 0.0), axis=1, keepdims=True)
    norm_before = scalars_ref[0:1, 0:1]
    step_before = scalars_ref[1:2, 0:1]
    ratio = norm / norm_before
    step = norm / (cross - bent - ratio * norm / step_before)
    kept = first_ref[:, 0:1] - step_before * second_ref[:, 0:1] - step * (column + ratio * second_ref[:, 0:1])
    coarse = own_part(spread_planes(kept, ids_ref)[1], cy, cz)

    def finish(p, value):
        at = p - HALO
        before = own_part(residual_ref[p], cy, cz)
        now = next_ref[at]
        along = product_ref[at] - own_part(value, cy, cz) + ratio * along_ref[at]
        final_ref[at] = now - step * along
        solution_ref[at] = coarse + step_before * before + step * (now + ratio * before)

    operate(by_plane(spread_planes(column, ids_ref), cx), weights_ref, HALO, planes - HALO, finish)


def call(kernel, name, outs, args, specs=None, scratch=()):
    return pl.pallas_call(
        kernel,
        name=name,
        out_shape=[jax.ShapeDtypeStruct(shape, jnp.float32) for shape in outs],
        in_specs=specs or [VMEM] * len(args),
        out_specs=[VMEM] * len(outs),
        scratch_shapes=[pltpu.VMEM(shape, jnp.float32) for shape in scratch],
    )(*args)


def both_sides(cells, axis, dim, width):
    count = lax.axis_size(axis)
    size = cells.shape[dim]
    head = lax.slice_in_dim(cells, 0, width, axis=dim)
    tail = lax.slice_in_dim(cells, size - width, size, axis=dim)
    before = lax.ppermute(tail, axis, [(i, i + 1) for i in range(count - 1)])
    after = lax.ppermute(head, axis, [(i + 1, i) for i in range(count - 1)])
    return before, after


def exchanged(rows, axes):
    return lax.all_to_all(rows, axes, 0, 0)


def summed(rows, gxy):
    row = jnp.sum(exchanged(rows, "gz"), axis=0, keepdims=True)
    return exchanged(jnp.broadcast_to(row, (gxy, 1, LANES)), ("gx", "gy"))


def body(right_side, fiber_class, conductivity_scale, class_tensor, block_ids):
    cx, cy, cz = right_side.shape
    gx, gy, gz = (lax.axis_size(a) for a in ("gx", "gy", "gz"))
    gxy, half = gx * gy, gz // 2
    place_x, place_y, place_z = (lax.axis_index(a) for a in ("gx", "gy", "gz"))

    (rows,) = call(
        own_sums_kernel, "own_sums", [(gz, 1, LANES)],
        [class_tensor, right_side, fiber_class, conductivity_scale, jnp.asarray(crossing_table())],
        specs=[SMEM, VMEM, VMEM, VMEM, VMEM], scratch=[(ROWS, cz)],
    )
    rows = exchanged(rows, "gz").reshape(gz, LANES)[:, : ZBLK * SLOTS]
    rows = jnp.concatenate([rows[:half], rows[half:]], axis=1)
    rows = exchanged(jnp.broadcast_to(rows[None], (gxy, half, LANES)), ("gx", "gy"))

    padded_ids = jnp.pad(block_ids, 1, constant_values=-1)
    shown = jnp.stack(
        [padded_ids[1 + a : 1 + a + gx, 1 + b : 1 + b + gy, 1 + c : 1 + c + gz * ZBLK] for a, b, c in ((0, 0, 0),) + NEIGHBOURS]
    )
    shown = shown.reshape(NNB + 1, gxy, 2, half, ZBLK)
    shown = jnp.transpose(shown, (2, 4, 0, 1, 3)).reshape(2 * ZBLK, NNB + 1, gxy * half)
    ids_all, near = shown[:, 0], shown[:, 1:]
    window = lax.dynamic_slice(padded_ids, (place_x, place_y, place_z * ZBLK), (3, 3, ZBLK + 2)).reshape(9, ZBLK + 2)
    block = cz // ZBLK
    ids = jnp.concatenate(
        [jnp.broadcast_to(window[:, 1 + j : 2 + j], (9, block)) for j in range(ZBLK)]
        + [
            jnp.broadcast_to(window[:, ZBLK + 1 :], (9, HALO)),
            jnp.full((9, EZ - cz - 2 * HALO), -1, jnp.int32),
            jnp.broadcast_to(window[:, :1], (9, HALO)),
        ],
        axis=1,
    )

    stacked = jnp.stack([right_side, fiber_class.astype(jnp.float32), conductivity_scale])
    before, after = both_sides(stacked, "gx", 1, HALO)
    stacked = jnp.concatenate([before, stacked, after], axis=1)
    before, after = both_sides(stacked, "gy", 2, HALO)
    gap = jnp.zeros((3, cx + 2 * HALO, EY - cy - 2 * HALO, cz), jnp.float32)
    stacked = jnp.concatenate([stacked, after, gap, before], axis=2)
    before, after = both_sides(stacked, "gz", 3, HALO)
    gap = jnp.zeros((3, cx + 2 * HALO, EY, EZ - cz - 2 * HALO), jnp.float32)
    stacked = jnp.concatenate([stacked, after, gap, before], axis=3)
    source, kinds, scale = stacked[0], stacked[1].astype(jnp.int32), stacked[2]
    extended = source.shape
    (weights,) = call(
        weights_kernel, "weights", [(len(EDGES),) + extended], [class_tensor, kinds, scale],
        specs=[SMEM, VMEM, VMEM], scratch=[(6,) + extended],
    )

    inverse, rhs = call(coarse_kernel, "coarse", [(COARSE, LANES), (1, LANES)], [rows, ids_all, near])
    residual, image, rows, first = call(
        first_kernel, "first", [extended, extended, (gz, 1, LANES), (COARSE, LANES)],
        [weights, source, scale, ids, inverse, rhs],
    )
    sums = summed(rows, gxy)
    following, product, along, rows, second, scalars = call(
        second_kernel, "second",
        [(cx, cy, cz)] * 3 + [(gz, 1, LANES), (COARSE, LANES), (8, LANES)],
        [weights, scale, residual, image, ids, inverse, sums],
        scratch=[extended],
    )
    sums = summed(rows, gxy)
    answer, final = call(
        last_kernel, "last", [(cx, cy, cz)] * 2,
        [weights, residual, following, product, along, ids, inverse, sums, scalars, first, second],
    )
    return answer, final


def solution(mesh):
    spec = P("gx", "gy", "gz")
    return jax.shard_map(
        body,
        mesh=mesh,
        in_specs=(spec, spec, spec, P(), P()),
        out_specs=(spec, spec),
        check_vma=False,
    )
```

```python
import functools

import jax
import jax.numpy as jnp
import numpy as np
from jax import lax
from jax.experimental import pallas as pl
from jax.experimental.pallas import tpu as pltpu
from jax.sharding import PartitionSpec as P

COARSE = 64
NCLS = 16
ZBLK = 2
HALO = 3
LANES = 128
EY = 24
EZ = 256
SLOTS = 32
HIGHEST = lax.Precision.HIGHEST

STENCIL_TAPS = (
    (1, 0, 0, 0, 1.0),
    (-1, 0, 0, 0, 1.0),
    (0, 1, 0, 1, 1.0),
    (0, -1, 0, 1, 1.0),
    (0, 0, 1, 2, 1.0),
    (0, 0, -1, 2, 1.0),
    (1, 1, 0, 3, 0.5),
    (-1, -1, 0, 3, 0.5),
    (1, -1, 0, 3, -0.5),
    (-1, 1, 0, 3, -0.5),
    (1, 0, 1, 4, 0.5),
    (-1, 0, -1, 4, 0.5),
    (1, 0, -1, 4, -0.5),
    (-1, 0, 1, 4, -0.5),
    (0, 1, 1, 5, 0.5),
    (0, -1, -1, 5, 0.5),
    (0, 1, -1, 5, -0.5),
    (0, -1, 1, 5, -0.5),
)
EDGES = (
    (1, 0, 0, 0, 1.0),
    (0, 1, 0, 1, 1.0),
    (0, 0, 1, 2, 1.0),
    (1, 1, 0, 3, 0.5),
    (1, -1, 0, 3, -0.5),
    (1, 0, 1, 4, 0.5),
    (1, 0, -1, 4, -0.5),
    (0, 1, 1, 5, 0.5),
    (0, 1, -1, 5, -0.5),
)
NEIGHBOURS = tuple(
    (a, b, c)
    for a in (-1, 0, 1)
    for b in (-1, 0, 1)
    for c in (-1, 0, 1)
    if 1 <= abs(a) + abs(b) + abs(c) <= 2
)
NNB = len(NEIGHBOURS)
RHS_SLOT = NNB
ROWS = 56
VMEM = pl.BlockSpec(memory_space=pltpu.VMEM)
SMEM = pl.BlockSpec(memory_space=pltpu.SMEM)


def crossing_table():
    table = np.zeros((3, SLOTS, ROWS), np.float32)

    def cells(step, reach):
        if step == 0:
            return ((2, 1.0),) if reach == 0 else ()
        edge = 1 if step > 0 else 0
        if reach == step:
            return ((edge, 1.0),)
        return ((2, 1.0), (edge, -1.0)) if reach == 0 else ()

    for sx, sy, sz, component, factor in STENCIL_TAPS:
        for slot, (a, b, c) in enumerate(NEIGHBOURS):
            for px, fx in cells(sx, a):
                for py, fy in cells(sy, b):
                    for pz, fz in cells(sz, c):
                        table[pz, slot, component * 9 + px * 3 + py] += 0.5 * factor * fx * fy * fz
    table[2, RHS_SLOT, 54] = 1.0
    return table.reshape(3 * SLOTS, ROWS)


def lookup(kinds, scale, table):
    values = [jnp.full(scale.shape, table[c, 0], jnp.float32) for c in range(6)]
    for kind in range(1, NCLS):
        hit = kinds == kind
        values = [jnp.where(hit, table[c, kind], values[c]) for c in range(6)]
    return [value * scale for value in values]


def lane_ids(shape):
    return lax.broadcasted_iota(jnp.int32, shape, len(shape) - 1)


def row_ids(shape):
    return lax.broadcasted_iota(jnp.int32, shape, len(shape) - 2)


def own_sums_kernel(table_ref, source_ref, kinds_ref, scale_ref, crossing_ref,
                    out_ref, stacked_ref, head_ref, tail_ref, rows_ref):
    cx, cy, cz = source_ref.shape
    for f, field in enumerate((source_ref, kinds_ref, scale_ref)):
        cells = field[...].astype(jnp.float32)
        stacked_ref[f] = cells
        head_ref[f] = cells[:HALO]
        tail_ref[f] = cells[cx - HALO :]
    rows_ref[...] = jnp.zeros_like(rows_ref)
    firsts, totals = None, None
    total_source = None
    for x in range(cx):
        layers = lookup(kinds_ref[x], scale_ref[x], table_ref)
        total_source = source_ref[x] if x == 0 else total_source + source_ref[x]
        if x == 0:
            firsts, totals = layers, layers
        else:
            totals = [t + v for t, v in zip(totals, layers)]
    for c in range(6):
        for px, field in enumerate((firsts[c], layers[c], totals[c])):
            at = c * 9 + px * 3
            rows_ref[at : at + 1, :] = field[0:1]
            rows_ref[at + 1 : at + 2, :] = field[cy - 1 : cy]
            rows_ref[at + 2 : at + 3, :] = jnp.sum(field, axis=0, keepdims=True)
    rows_ref[54:55, :] = jnp.sum(total_source, axis=0, keepdims=True)
    sums = jnp.dot(crossing_ref[...], rows_ref[...], precision=HIGHEST, preferred_element_type=jnp.float32)
    block = cz // ZBLK
    lane = lane_ids((SLOTS, cz))
    picked = (
        jnp.where(lane % block == 0, sums[:SLOTS], 0.0)
        + jnp.where(lane % block == block - 1, sums[SLOTS : 2 * SLOTS], 0.0)
        + sums[2 * SLOTS :]
    )
    spread = jnp.concatenate([picked] * ZBLK + [jnp.zeros((LANES - ZBLK * SLOTS, cz), jnp.float32)], axis=0)
    group = row_ids((LANES, cz)) // SLOTS
    spread = jnp.where(lane_ids((LANES, cz)) // block == group, spread, 0.0)
    row = lax.dot_general(
        jnp.ones((8, cz), jnp.float32), spread, (((1,), (1,)), ((), ())),
        precision=HIGHEST, preferred_element_type=jnp.float32,
    )
    out_ref[...] = jnp.broadcast_to(row[0:1].reshape(1, 1, LANES), out_ref.shape)


def shift_z(x, step):
    return pltpu.roll(x, (-step) % EZ, 1)


def shift_y(x, step):
    return pltpu.roll(x, (-step) % EY, 0)


def widen_kernel(rows_ref, out_ref):
    half = out_ref.shape[1]
    rows = rows_ref[...].reshape(2 * half, LANES)
    rows = rows[:half] + pltpu.roll(rows[half:], LANES // 2, 1)
    out_ref[...] = jnp.broadcast_to(rows[None], out_ref.shape)


def labels_kernel(block_ref, own_ref, near_ref, window_ref, flat_ref):
    gx, gy, nz = block_ref.shape
    gxy, half = gx * gy, nz // (2 * ZBLK)
    count = gxy * half
    for x in range(gx):
        flat_ref[x * gy : (x + 1) * gy, :] = block_ref[x].astype(jnp.float32) + 1.0
    flat = flat_ref[...]
    lane = lane_ids((gxy, count))
    row = row_ids((gxy, count))
    lane_x, lane_y = lane // half // gy, lane // half % gy
    depth = row_ids((nz, count))
    lane_r = lane_ids((nz, count)) % half
    own_ref[...] = jnp.zeros_like(own_ref)
    near_ref[...] = jnp.zeros_like(near_ref)
    for a in (-1, 0, 1):
        for b in (-1, 0, 1):
            steps = [c for c in (-1, 0, 1) if abs(a) + abs(b) + abs(c) <= 2]
            hit = (row == (lane_x + a) * gy + lane_y + b) & (lane_x + a >= 0) & (lane_x + a < gx)
            hit = hit & (lane_y + b >= 0) & (lane_y + b < gy)
            columns = lax.dot_general(
                flat, jnp.where(hit, 1.0, 0.0), (((0,), (0,)), ((), ())),
                precision=HIGHEST, preferred_element_type=jnp.float32,
            )
            for g in range(2 * ZBLK):
                level = ZBLK * (g // ZBLK * half + lane_r) + g % ZBLK
                for c in steps:
                    found = jnp.sum(jnp.where(depth == level + c, columns, 0.0), axis=0, keepdims=True)
                    found = (found + 0.5).astype(jnp.int32) - 1
                    if (a, b, c) == (0, 0, 0):
                        own_ref[g : g + 1, :] = found
                    else:
                        s = NEIGHBOURS.index((a, b, c))
                        near_ref[g, s : s + 1, :] = found
    place_x, place_y, place_z = (lax.axis_index(n) for n in ("gx", "gy", "gz"))
    at = row_ids((16, gxy))
    beside_x, beside_y = place_x + at // 3 - 1, place_y + at % 3 - 1
    hit = (lane_ids((16, gxy)) == beside_x * gy + beside_y) & (beside_x >= 0) & (beside_x < gx)
    hit = hit & (beside_y >= 0) & (beside_y < gy) & (at < 9)
    picked = jnp.dot(jnp.where(hit, 1.0, 0.0), flat, precision=HIGHEST, preferred_element_type=jnp.float32)
    lane = lane_ids((nz, EZ))
    level = ZBLK * place_z + jnp.where(
        lane < LANES, lane // (LANES // ZBLK), jnp.where(lane < LANES + HALO, ZBLK, -1)
    )
    hit = (row_ids((nz, EZ)) == level) & ((lane < LANES + HALO) | (lane >= EZ - HALO))
    window = jnp.dot(picked, jnp.where(hit, 1.0, 0.0), precision=HIGHEST, preferred_element_type=jnp.float32)
    window_ref[...] = (window + 0.5).astype(jnp.int32) - 1


def fill_weights(table_ref, stacked_ref, out_ref):
    planes = stacked_ref.shape[1]

    def layers_of(p):
        layers = lookup(stacked_ref[1, p], stacked_ref[2, p], table_ref)
        return [(0.5 if c < 3 else 0.25) * layer for c, layer in enumerate(layers)]

    here = layers_of(0)
    for p in range(planes):
        after = layers_of(p + 1) if p + 1 < planes else here
        up = shift_y(here[5], 1)
        out_ref[0, p] = here[0] + after[0]
        out_ref[1, p] = here[1] + shift_y(here[1], 1)
        out_ref[2, p] = here[2] + shift_z(here[2], 1)
        out_ref[3, p] = here[3] + shift_y(after[3], 1)
        out_ref[4, p] = -(here[3] + shift_y(after[3], -1))
        out_ref[5, p] = here[4] + shift_z(after[4], 1)
        out_ref[6, p] = -(here[4] + shift_z(after[4], -1))
        out_ref[7, p] = here[5] + shift_z(up, 1)
        out_ref[8, p] = -(here[5] + shift_z(up, -1))
        here = after


def inside_mask(sides_ref):
    row, lane = row_ids((EY, EZ)), lane_ids((EY, EZ))
    cy = EY - 8
    rows = (row < cy) | ((row < cy + HALO) & (sides_ref[3] > 0)) | ((row >= EY - HALO) & (sides_ref[2] > 0))
    lanes = (lane < LANES) | ((lane < LANES + HALO) & (sides_ref[5] > 0)) | ((lane >= EZ - HALO) & (sides_ref[4] > 0))
    return rows & lanes


def inside_plane(mask, p, cx, sides_ref):
    if p < HALO:
        return mask & (sides_ref[0] > 0)
    if p >= HALO + cx:
        return mask & (sides_ref[1] > 0)
    return mask


def across(here, after, weights, p):
    g1 = weights[0, p] * (here - after)
    g2 = weights[3, p] * (here - shift_y(after, 1))
    g3 = weights[4, p] * (here - shift_y(after, -1))
    g4 = weights[5, p] * (here - shift_z(after, 1))
    g5 = weights[6, p] * (here - shift_z(after, -1))
    leaving = (g1 + g2) + (g3 + g4) + g5
    arriving = (g1 + shift_y(g2, -1)) + (shift_y(g3, 1) + shift_z(g4, -1)) + shift_z(g5, 1)
    return leaving, arriving


def within(here, weights, p):
    up = shift_y(here, 1)
    h1 = weights[1, p] * (here - up)
    h2 = weights[2, p] * (here - shift_z(here, 1))
    h3 = weights[7, p] * (here - shift_z(up, 1))
    h4 = weights[8, p] * (here - shift_z(up, -1))
    back = shift_y(h1 + shift_z(h3, -1) + shift_z(h4, 1), -1) + shift_z(h2, -1)
    return (h1 + h2) + (h3 + h4) - back


def operate(plane, weights, low, high, emit):
    _, arriving = across(plane(low - 1), plane(low), weights, low - 1)
    for p in range(low, high):
        here = plane(p)
        leaving, coming = across(here, plane(p + 1), weights, p)
        emit(p, within(here, weights, p) + leaving - arriving)
        arriving = coming


def column_of(inverse, row):
    return jnp.sum(inverse * row, axis=1, keepdims=True)


def spread_planes(column, ids_ref):
    coarse = column.shape[0]
    wide = jnp.broadcast_to(column, (coarse, EZ))
    label = row_ids((coarse, EZ))
    row = row_ids((EY, EZ))
    cy = EY - 8
    planes = []
    for a in range(3):
        before, own, after = (
            jnp.sum(jnp.where(ids_ref[3 * a + b : 3 * a + b + 1, :] == label, wide, 0.0), axis=0, keepdims=True)
            for b in range(3)
        )
        planes.append(jnp.where(row < cy, own, jnp.where(row < cy + 4, after, before)))
    return planes


def by_plane(planes, cx):
    return lambda p: planes[0] if p < HALO else planes[1] if p < HALO + cx else planes[2]


def labelled_row(totals, norm, cross, ids_ref):
    lane = lane_ids((1, LANES))
    block = LANES // ZBLK
    row = jnp.where(lane == COARSE, jnp.sum(norm, keepdims=True).reshape(1, 1), 0.0)
    row = row + jnp.where(lane == COARSE + 1, jnp.sum(cross, keepdims=True).reshape(1, 1), 0.0)
    for j in range(ZBLK):
        total = jnp.sum(jnp.where(lane // block == j, totals, 0.0), axis=1, keepdims=True)
        label = ids_ref[4:5, j * block : j * block + 1]
        row = row + jnp.where(lane == label, total, 0.0)
    return row


def own_part(plane, cy, cz):
    return plane[:cy, :cz]


def coarse_kernel(rows_ref, ids_ref, near_ref, inverse_ref, rhs_ref):
    count = rows_ref.shape[0] * rows_ref.shape[1]
    flat = rows_ref[...].reshape(count, LANES)
    features = flat.T
    coarse = inverse_ref.shape[0]
    label = row_ids((coarse, count))
    slot_row = row_ids((SLOTS, count))
    packed = None
    for g in range(LANES // SLOTS):
        part = features[g * SLOTS : (g + 1) * SLOTS]
        reach = None
        for s in range(NNB):
            term = jnp.where(near_ref[g, s : s + 1, :] == label, part[s : s + 1], 0.0)
            reach = term if s == 0 else reach + term
        crossing = jnp.sum(jnp.where(slot_row < NNB, part, 0.0), axis=0, keepdims=True)
        sub = row_ids((8, count))
        extra = jnp.where(sub == 0, crossing, jnp.where(sub == 1, part[RHS_SLOT : RHS_SLOT + 1], 0.0))
        own = jnp.where(ids_ref[g : g + 1, :] == label, 1.0, 0.0)
        product = lax.dot_general(
            jnp.concatenate([reach, extra], axis=0), own, (((1,), (1,)), ((), ())),
            precision=HIGHEST, preferred_element_type=jnp.float32,
        )
        packed = product if g == 0 else packed + product
    coupling = packed[:coarse]
    mirrored = coupling.T
    row = row_ids((coarse, coarse))
    lane = lane_ids((coarse, coarse))
    diagonal = packed[coarse : coarse + 1] + jnp.sum(mirrored, axis=0, keepdims=True)
    matrix = jnp.where(row == lane, diagonal, 0.0) - (coupling + mirrored)
    panel = 8
    for start in range(0, coarse, panel):
        columns = [
            jnp.broadcast_to(matrix[:, k : k + 1], (coarse, coarse)) for k in range(start, start + panel)
        ]
        for i in range(panel):
            k = start + i
            column = columns[i]
            inverse_pivot = 1.0 / column[k : k + 1, :]
            scaled = matrix[k : k + 1, :] * inverse_pivot
            scaled = jnp.where(lane[:1] == k, inverse_pivot, scaled)
            matrix = jnp.where(lane == k, 0.0, matrix) - column * scaled
            matrix = jnp.where(row == k, scaled, matrix)
            for m in range(i + 1, panel):
                factor = columns[m][k : k + 1, :] * inverse_pivot
                columns[m] = jnp.where(row == k, factor, columns[m] - column * factor)
    inverse_ref[...] = jnp.concatenate([matrix, jnp.zeros((coarse, LANES - coarse), jnp.float32)], axis=1)
    rhs_ref[...] = jnp.concatenate(
        [packed[coarse + 1 : coarse + 2], jnp.zeros((1, LANES - coarse), jnp.float32)], axis=1
    )


def first_kernel(table_ref, sides_ref, stacked_ref, ids_ref, inverse_ref, rhs_ref,
                 weights_ref, residual_ref, image_ref, row_ref, column_ref):
    planes = stacked_ref.shape[1]
    cx, cy, cz = planes - 2 * HALO, EY - 8, LANES
    fill_weights(table_ref, stacked_ref, weights_ref)
    mask = inside_mask(sides_ref)
    column = column_of(inverse_ref[...], rhs_ref[...])
    column_ref[...] = jnp.broadcast_to(column, column_ref.shape)
    residual_ref[0] = jnp.zeros((EY, EZ), jnp.float32)
    residual_ref[planes - 1] = jnp.zeros((EY, EZ), jnp.float32)

    def residual(p, image):
        residual_ref[p] = jnp.where(inside_plane(mask, p, cx, sides_ref), stacked_ref[0, p] - image, 0.0)

    operate(by_plane(spread_planes(column, ids_ref), cx), weights_ref, 1, planes - 1, residual)
    sums = [jnp.zeros((cy, cz), jnp.float32)] * 3

    def image(p, value):
        image_ref[p] = value
        if HALO <= p < HALO + cx:
            mine, field = own_part(value, cy, cz), own_part(residual_ref[p], cy, cz)
            sums[0] = sums[0] + mine
            sums[1] = sums[1] + field * field
            sums[2] = sums[2] + field * mine

    operate(lambda p: residual_ref[p], weights_ref, 2, planes - 2, image)
    row = labelled_row(jnp.sum(sums[0], axis=0, keepdims=True), sums[1], sums[2], ids_ref)
    row_ref[...] = jnp.broadcast_to(row.reshape(1, 1, LANES), row_ref.shape)


def second_kernel(sides_ref, weights_ref, residual_ref, image_ref, ids_ref, inverse_ref, sums_ref,
                  next_ref, product_ref, along_ref, row_ref, column_ref, scalars_ref, field_ref):
    planes = residual_ref.shape[0]
    cx, cy, cz = planes - 2 * HALO, EY - 8, LANES
    mask = inside_mask(sides_ref)
    totals = jnp.sum(sums_ref[...], axis=0)
    column = column_of(inverse_ref[...], totals)
    column_ref[...] = jnp.broadcast_to(column, column_ref.shape)
    lane = lane_ids((1, LANES))
    inverse = inverse_ref[...]
    bent = jnp.sum(column * jnp.sum(jnp.where(lane_ids(inverse.shape) == row_ids(inverse.shape), totals, 0.0), axis=1, keepdims=True), axis=0, keepdims=True)
    norm = jnp.sum(jnp.where(lane == COARSE, totals, 0.0), axis=1, keepdims=True)
    cross = jnp.sum(jnp.where(lane == COARSE + 1, totals, 0.0), axis=1, keepdims=True)
    step = norm / (cross - bent)
    sub = row_ids((8, LANES))
    scalars_ref[...] = jnp.where(sub == 0, norm, jnp.where(sub == 1, step, 0.0))

    def follow(p, value):
        value = image_ref[p] - value
        if HALO <= p < HALO + cx:
            along_ref[p - HALO] = own_part(value, cy, cz)
        updated = jnp.where(inside_plane(mask, p, cx, sides_ref), residual_ref[p] - step * value, 0.0)
        field_ref[p] = updated
        if HALO <= p < HALO + cx:
            next_ref[p - HALO] = own_part(updated, cy, cz)

    operate(by_plane(spread_planes(column, ids_ref), cx), weights_ref, 2, planes - 2, follow)
    sums = [jnp.zeros((cy, cz), jnp.float32)] * 3

    def image(p, value):
        mine, field = own_part(value, cy, cz), own_part(field_ref[p], cy, cz)
        product_ref[p - HALO] = mine
        sums[0] = sums[0] + mine
        sums[1] = sums[1] + field * field
        sums[2] = sums[2] + field * mine

    operate(lambda p: field_ref[p], weights_ref, HALO, planes - HALO, image)
    row = labelled_row(jnp.sum(sums[0], axis=0, keepdims=True), sums[1], sums[2], ids_ref)
    row_ref[...] = jnp.broadcast_to(row.reshape(1, 1, LANES), row_ref.shape)


def last_kernel(weights_ref, residual_ref, next_ref, product_ref, along_ref, ids_ref, inverse_ref, sums_ref,
                scalars_ref, first_ref, second_ref, solution_ref, final_ref):
    cx, cy, cz = next_ref.shape
    planes = cx + 2 * HALO
    totals = jnp.sum(sums_ref[...], axis=0)
    inverse = inverse_ref[...]
    column = column_of(inverse, totals)
    lane = lane_ids((1, LANES))
    bent = jnp.sum(column * jnp.sum(jnp.where(lane_ids(inverse.shape) == row_ids(inverse.shape), totals, 0.0), axis=1, keepdims=True), axis=0, keepdims=True)
    norm = jnp.sum(jnp.where(lane == COARSE, totals, 0.0), axis=1, keepdims=True)
    cross = jnp.sum(jnp.where(lane == COARSE + 1, totals, 0.0), axis=1, keepdims=True)
    norm_before = scalars_ref[0:1, 0:1]
    step_before = scalars_ref[1:2, 0:1]
    ratio = norm / norm_before
    step = norm / (cross - bent - ratio * norm / step_before)
    kept = first_ref[:, 0:1] - step_before * second_ref[:, 0:1] - step * (column + ratio * second_ref[:, 0:1])
    coarse = own_part(spread_planes(kept, ids_ref)[1], cy, cz)

    def finish(p, value):
        at = p - HALO
        before = own_part(residual_ref[p], cy, cz)
        now = next_ref[at]
        along = product_ref[at] - own_part(value, cy, cz) + ratio * along_ref[at]
        final_ref[at] = now - step * along
        solution_ref[at] = coarse + step_before * before + step * (now + ratio * before)

    operate(by_plane(spread_planes(column, ids_ref), cx), weights_ref, HALO, planes - HALO, finish)


def call(kernel, outs, args, specs=None, scratch=()):
    return pl.pallas_call(
        kernel,
        out_shape=[
            shape if isinstance(shape, jax.ShapeDtypeStruct) else jax.ShapeDtypeStruct(shape, jnp.float32)
            for shape in outs
        ],
        in_specs=specs or [VMEM] * len(args),
        out_specs=[VMEM] * len(outs),
        scratch_shapes=[pltpu.VMEM(shape, jnp.float32) for shape in scratch],
        compiler_params=pltpu.CompilerParams(vmem_limit_bytes=16 * 2**20),
    )(*args)


def both_sides(head, tail, axis):
    count = lax.axis_size(axis)
    before = lax.ppermute(tail, axis, [(i, i + 1) for i in range(count - 1)])
    after = lax.ppermute(head, axis, [(i + 1, i) for i in range(count - 1)])
    return before, after


def exchanged(rows, axes):
    return lax.all_to_all(rows, axes, 0, 0)


def summed(rows, gxy):
    row = jnp.sum(exchanged(rows, "gz"), axis=0, keepdims=True)
    return exchanged(jnp.broadcast_to(row, (gxy, 1, LANES)), ("gx", "gy"))


def body(right_side, fiber_class, conductivity_scale, class_tensor, block_ids):
    cx, cy, cz = right_side.shape
    gx, gy, gz = (lax.axis_size(a) for a in ("gx", "gy", "gz"))
    gxy, half = gx * gy, gz // 2
    slab = (3, HALO, cy, cz)
    rows, stacked, head, tail = call(
        own_sums_kernel, [(gz, 1, LANES), (3, cx, cy, cz), slab, slab],
        [class_tensor, right_side, fiber_class, conductivity_scale, jnp.asarray(crossing_table())],
        specs=[SMEM, VMEM, VMEM, VMEM, VMEM], scratch=[(ROWS, cz)],
    )
    rows = exchanged(rows, "gz")
    (rows,) = call(widen_kernel, [(gxy, half, LANES)], [rows])
    rows = exchanged(rows, ("gx", "gy"))

    whole = functools.partial(jax.ShapeDtypeStruct, dtype=jnp.int32)
    ids_all, near, ids = call(
        labels_kernel,
        [whole((8, gxy * half)), whole((2 * ZBLK, 24, gxy * half)), whole((16, EZ))],
        [block_ids], scratch=[(gxy, gz * ZBLK)],
    )

    before, after = both_sides(head, tail, "gx")
    stacked = jnp.concatenate([before, stacked, after], axis=1)
    before, after = both_sides(stacked[:, :, :HALO], stacked[:, :, cy - HALO :], "gy")
    gap = jnp.zeros((3, cx + 2 * HALO, EY - cy - 2 * HALO, cz), jnp.float32)
    stacked = jnp.concatenate([stacked, after, gap, before], axis=2)
    before, after = both_sides(stacked[..., :HALO], stacked[..., cz - HALO :], "gz")
    gap = jnp.zeros((3, cx + 2 * HALO, EY, EZ - cz - 2 * HALO), jnp.float32)
    stacked = jnp.concatenate([stacked, after, gap, before], axis=3)
    extended = stacked.shape[1:]
    places = [lax.axis_index(a) for a in ("gx", "gy", "gz")]
    sides = jnp.stack(
        [jnp.int32(f) for place, count in zip(places, (gx, gy, gz)) for f in (place > 0, place < count - 1)]
    )

    inverse, rhs = call(coarse_kernel, [(COARSE, LANES), (1, LANES)], [rows, ids_all, near])
    weights, residual, image, rows, first = call(
        first_kernel,
        [(len(EDGES),) + extended, extended, extended, (gz, 1, LANES), (COARSE, LANES)],
        [class_tensor, sides, stacked, ids, inverse, rhs],
        specs=[SMEM, SMEM, VMEM, VMEM, VMEM, VMEM],
    )
    sums = summed(rows, gxy)
    following, product, along, rows, second, scalars = call(
        second_kernel,
        [(cx, cy, cz)] * 3 + [(gz, 1, LANES), (COARSE, LANES), (8, LANES)],
        [sides, weights, residual, image, ids, inverse, sums],
        specs=[SMEM] + [VMEM] * 6,
        scratch=[extended],
    )
    sums = summed(rows, gxy)
    answer, final = call(
        last_kernel, [(cx, cy, cz)] * 2,
        [weights, residual, following, product, along, ids, inverse, sums, scalars, first, second],
    )
    return answer, final


def solution(mesh):
    spec = P("gx", "gy", "gz")
    return jax.shard_map(
        body,
        mesh=mesh,
        in_specs=(spec, spec, spec, P(), P()),
        out_specs=(spec, spec),
        check_vma=False,
    )
```
